128 devices in a mesh: data: 1, feat: 2 (over core), graph: 64 (over z, y, x).
Axes of the slice: x: 4, y: 4, z: 4, core: 2. Of those that a mesh axis runs over, the one named last changes fastest.
Arguments:
- X: bfloat16 [131072, 100], P(('data', 'graph'), 'feat')
- dst_local: int32 [6553600], P(('data', 'graph'))
- src_slot: int32 [6553600], P(('data', 'graph'))
- valid: int32 [6553600], P(('data', 'graph'))
- w: float32 [6553600], P(('data', 'graph'))
- send_idx: int32 [4096, 32], P(('data', 'graph'))
- send_valid: int32 [4096, 32], P(('data', 'graph'))
- hub_ids: int32 [1024], P('data')
- W1: bfloat16 [100, 256], P('feat')
- W2: bfloat16 [256, 256], P('feat')
- b1: float32 [256], P('feat')
- b2: float32 [256], P('feat')
Outputs:
- output: float32 [131072, 256], P(('data', 'graph'), 'feat')
All inputs are finite; a program needn't handle non-finite values.
Results may differ from the reference program's by a relative error of at most 0.001.
Values are sent between devices in bfloat16 or wider.
A program may use at most 1 GiB of HBM per device.

```python
import jax
import jax.numpy as jnp
from jax import lax

GRAPH = 64
VERT_DEV = 2048
DEG = 50
SEND_ROWS = 32
F_IN = 100
F_HID = 256

HUB_DEV = VERT_DEV // 128
HUB_COUNT = GRAPH * HUB_DEV
EDGE_DEV = VERT_DEV * DEG
ACC_ROWS = VERT_DEV + HUB_COUNT


def draw_graph(key):
    sub_keys = jax.random.split(key, 12)
    nonhub = VERT_DEV - HUB_DEV
    dev_ids = jnp.arange(GRAPH)
    row_perm = jax.vmap(lambda sub_key: jax.random.permutation(sub_key, VERT_DEV))(jax.random.split(sub_keys[0], GRAPH))
    hub_ids = (dev_ids[:, None] * VERT_DEV + row_perm[:, :HUB_DEV]).reshape(HUB_COUNT)
    edge_count = jax.random.randint(sub_keys[1], (GRAPH,), EDGE_DEV // 4, EDGE_DEV + 1)
    full_dev = jax.random.randint(sub_keys[2], (), 0, GRAPH)
    edge_count = jnp.where(dev_ids == full_dev, EDGE_DEV, edge_count)
    valid = (jnp.arange(EDGE_DEV)[None, :] < edge_count[:, None]).astype(jnp.int32)
    send_count = jax.random.randint(sub_keys[3], (GRAPH, GRAPH), max(1, SEND_ROWS // 4), SEND_ROWS + 1)
    full_pair = jax.random.randint(sub_keys[4], (), 0, GRAPH)
    is_full = (dev_ids[:, None] == full_pair) & (dev_ids[None, :] == (full_pair + 1) % GRAPH)
    send_count = jnp.where(is_full, SEND_ROWS, send_count)
    send_count = jnp.where(dev_ids[:, None] == dev_ids[None, :], 0, send_count)
    send_valid = (jnp.arange(SEND_ROWS)[None, None, :] < send_count[:, :, None]).astype(jnp.int32)
    send_rank = jax.random.randint(sub_keys[5], (GRAPH, GRAPH, SEND_ROWS), 0, nonhub)
    send_idx = row_perm[dev_ids[:, None, None], HUB_DEV + send_rank]
    src_kind = jax.random.randint(sub_keys[6], (GRAPH, EDGE_DEV), 0, 100)
    local_src = jax.random.randint(sub_keys[7], (GRAPH, EDGE_DEV), 0, VERT_DEV)
    peer_dev = (dev_ids[:, None] + 1 + jax.random.randint(sub_keys[8], (GRAPH, EDGE_DEV), 0, GRAPH - 1)) % GRAPH
    peer_count = send_count[peer_dev, dev_ids[:, None]]
    halo_pos = jax.random.randint(sub_keys[9], (GRAPH, EDGE_DEV), 0, peer_count)
    halo_src = VERT_DEV + peer_dev * SEND_ROWS + halo_pos
    hub_src = VERT_DEV + GRAPH * SEND_ROWS + jax.random.randint(sub_keys[10], (GRAPH, EDGE_DEV), 0, HUB_COUNT)
    src_slot = jnp.where(src_kind < 50, local_src, jnp.where(src_kind < 85, halo_src, hub_src))
    dst_keys = jax.random.split(sub_keys[11], 3)
    dst_kind = jax.random.randint(dst_keys[0], (GRAPH, EDGE_DEV), 0, 100)
    skew_draw = jax.random.randint(dst_keys[1], (GRAPH, EDGE_DEV), 0, 32768)
    dst_rank = (((skew_draw * skew_draw) >> 15) * nonhub) >> 15
    local_dst = row_perm[dev_ids[:, None], HUB_DEV + dst_rank]
    hub_dst = VERT_DEV + jax.random.randint(dst_keys[2], (GRAPH, EDGE_DEV), 0, HUB_COUNT)
    dst_local = jnp.where(dst_kind < 10, hub_dst, local_dst)
    flat_dst = (dev_ids[:, None] * ACC_ROWS + dst_local).reshape(-1)
    in_deg = jax.ops.segment_sum(valid.reshape(-1), flat_dst, num_segments=GRAPH * ACC_ROWS).reshape(GRAPH, ACC_ROWS)
    hub_deg = jnp.sum(in_deg[:, VERT_DEV:], axis=0)
    all_deg = jnp.concatenate([in_deg[:, :VERT_DEV], jnp.broadcast_to(hub_deg[None, :], (GRAPH, HUB_COUNT))], axis=1)
    dst_deg = jnp.take_along_axis(all_deg, dst_local, axis=1)
    return dst_local, src_slot, valid, dst_deg, send_idx, send_valid, hub_ids


def setup_inputs(seed: int = 0, part: int = 0) -> dict:
    base_key = jax.random.key(seed)
    part_key = jax.random.fold_in(base_key, part)
    dst_local, src_slot, valid, dst_deg, send_idx, send_valid, hub_ids = draw_graph(jax.random.fold_in(part_key, 1))
    key_x, key_u = jax.random.split(jax.random.fold_in(part_key, 2), 2)
    key_w1, key_w2, key_b1, key_b2 = jax.random.split(jax.random.key(seed + 1), 4)
    feats = jax.random.normal(key_x, (GRAPH * VERT_DEV, F_IN), jnp.float32)
    edge_scale = jax.random.uniform(key_u, (GRAPH, EDGE_DEV), jnp.float32, 0.5, 1.5)
    edge_weight = edge_scale * lax.rsqrt(jnp.maximum(dst_deg, 1).astype(jnp.float32))
    w_first = jax.random.normal(key_w1, (F_IN, F_HID), jnp.float32) * (F_IN ** -0.5)
    w_second = jax.random.normal(key_w2, (F_HID, F_HID), jnp.float32) * (F_HID ** -0.5)
    return {
        "X": feats.astype(jnp.bfloat16),
        "dst_local": dst_local.reshape(-1),
        "src_slot": src_slot.reshape(-1),
        "valid": valid.reshape(-1),
        "w": edge_weight.reshape(-1),
        "send_idx": send_idx.reshape(GRAPH * GRAPH, SEND_ROWS),
        "send_valid": send_valid.reshape(GRAPH * GRAPH, SEND_ROWS),
        "hub_ids": hub_ids,
        "W1": w_first.astype(jnp.bfloat16),
        "W2": w_second.astype(jnp.bfloat16),
        "b1": 0.5 * jax.random.normal(key_b1, (F_HID,), jnp.float32),
        "b2": 0.5 * jax.random.normal(key_b2, (F_HID,), jnp.float32),
    }


def reference(X, dst_local, src_slot, valid, w, send_idx, send_valid, hub_ids, W1, W2, b1, b2):
    dst_dev = dst_local.reshape(GRAPH, EDGE_DEV)
    src_dev = src_slot.reshape(GRAPH, EDGE_DEV)
    coef_dev = (w * valid.astype(jnp.float32)).reshape(GRAPH, EDGE_DEV)
    send_grid = send_idx.reshape(GRAPH, GRAPH, SEND_ROWS)
    keep_grid = send_valid.reshape(GRAPH, GRAPH, SEND_ROWS) > 0
    sender_ids = jnp.arange(GRAPH)[:, None]

    def gcn_layer(layer_in, weight, bias_vec):
        z_rows = jnp.dot(layer_in, weight, preferred_element_type=jnp.float32).astype(jnp.bfloat16)
        feat_width = weight.shape[1]
        z_grid = z_rows.reshape(GRAPH, VERT_DEV, feat_width)
        hub_feat = z_rows[hub_ids]

        def device_sum(dev_args):
            dev_index, dst_edges, src_edges, coef_edges = dev_args
            halo_rows = z_grid[sender_ids, send_grid[:, dev_index, :]]
            halo_rows = jnp.where(keep_grid[:, dev_index, :, None], halo_rows, jnp.zeros_like(halo_rows))
            slot_table = jnp.concatenate([z_grid[dev_index], halo_rows.reshape(GRAPH * SEND_ROWS, feat_width), hub_feat], axis=0)
            messages = slot_table[src_edges].astype(jnp.float32) * coef_edges[:, None]
            return jax.ops.segment_sum(messages, dst_edges, num_segments=ACC_ROWS)

        partial_sum = lax.map(device_sum, (jnp.arange(GRAPH), dst_dev, src_dev, coef_dev))
        hub_total = jnp.sum(partial_sum[:, VERT_DEV:], axis=0)
        own_rows = partial_sum[:, :VERT_DEV].reshape(GRAPH * VERT_DEV, feat_width).at[hub_ids].add(hub_total)
        return own_rows + bias_vec

    hidden = jnp.maximum(gcn_layer(X, W1, b1), 0.0).astype(jnp.bfloat16)
    return gcn_layer(hidden, W2, b2)
```

```python
import functools

import jax
import jax.numpy as jnp
from jax import lax
from jax.experimental import pallas as pl
from jax.experimental.pallas import tpu as pltpu
from jax.sharding import PartitionSpec as P

DB = 128
SB = 256
CH = 256
UNROLL = 8
BF = jnp.bfloat16
F32 = jnp.float32


def split3(a):
    hi = a.astype(BF)
    rest = a - hi.astype(F32)
    mid = rest.astype(BF)
    low = (rest - mid.astype(F32)).astype(BF)
    return hi, mid, low


def block_product(a_ref, table_ref, y_ref):
    rows, depth = a_ref.shape
    total = jnp.zeros((3 * rows, table_ref.shape[1]), F32)
    for k in range(0, depth, SB):
        pieces = jnp.concatenate(split3(a_ref[:, k : k + SB]), axis=0)
        total = total + jnp.dot(pieces, table_ref[k : k + SB, :], preferred_element_type=F32)
    y_ref[...] = total[:rows] + total[rows : 2 * rows] + total[2 * rows :]


def build_kernel(n_src, kf_ref, kl_ref, key_ref, low_ref, w_ref, table_ref, a_ref, y_ref, state_ref):
    step = pl.program_id(0)
    n_chunks = key_ref.shape[0]

    @pl.when(step == 0)
    def _():
        state_ref[0] = 0
        state_ref[1] = kf_ref[0]

    first = step * n_src
    limit = first + n_src
    a_ref[...] = jnp.zeros_like(a_ref)

    def body(carry):
        chunk, bucket = carry
        for _ in range(UNROLL):
            live = bucket < limit
            here = jnp.minimum(chunk, n_chunks - 1)
            keys = key_ref[here]
            lows = low_ref[here]
            match = keys == jnp.where(live, bucket, -1)
            d_low = jnp.where(match, lax.shift_right_logical(lows, 8), -1)
            s_low = lows & (SB - 1)
            weights = w_ref[here]
            d_mask = lax.broadcasted_iota(jnp.int32, (DB, CH), 0) == d_low
            pieces = [jnp.where(d_mask, piece.astype(F32), 0.0).astype(BF) for piece in split3(weights)]
            s_hot = jnp.where(lax.broadcasted_iota(jnp.int32, (SB, CH), 0) == s_low, 1.0, 0.0).astype(BF)
            got = lax.dot_general(
                jnp.concatenate(pieces, axis=0), s_hot, (((1,), (1,)), ((), ())), preferred_element_type=F32
            )
            got = got[:DB] + got[DB : 2 * DB] + got[2 * DB :]
            column = pl.multiple_of(jnp.clip(bucket - first, 0, n_src - 1) * SB, SB)
            a_ref[:, pl.ds(column, SB)] += got
            done = bucket >= kl_ref[here]
            next_chunk = chunk + jnp.where(done, 1, 0)
            next_bucket = jnp.where(done, kf_ref[next_chunk], bucket + 1)
            chunk = jnp.where(live, next_chunk, chunk)
            bucket = jnp.where(live, next_bucket, bucket)
        return chunk, bucket

    chunk, bucket = lax.while_loop(lambda c: c[1] < limit, body, (state_ref[0], state_ref[1]))
    state_ref[0] = chunk
    state_ref[1] = bucket
    block_product(a_ref, table_ref, y_ref)


def build_and_multiply(key, low, w, table, n_dst):
    n_src = table.shape[0] // SB
    width = table.shape[1]
    n_chunks = key.shape[0] // CH
    keys = key.reshape(n_chunks, 1, CH)
    end = jnp.full((8,), n_dst * n_src, jnp.int32)
    k_first = jnp.concatenate([keys[:, 0, 0], end])
    k_last = jnp.concatenate([keys[:, 0, CH - 1], end])
    whole = lambda *shape: pl.BlockSpec(shape, lambda i, *_: (0,) * len(shape), pipeline_mode=pl.Buffered(1))
    return pl.pallas_call(
        functools.partial(build_kernel, n_src),
        grid_spec=pltpu.PrefetchScalarGridSpec(
            num_scalar_prefetch=2,
            grid=(n_dst,),
            in_specs=[whole(n_chunks, 1, CH)] * 3 + [whole(*table.shape)],
            out_specs=[
                pl.BlockSpec((DB, n_src * SB), lambda i, *_: (i, 0)),
                pl.BlockSpec((DB, width), lambda i, *_: (i, 0)),
            ],
            scratch_shapes=[pltpu.SMEM((2,), jnp.int32)],
        ),
        out_shape=[
            jax.ShapeDtypeStruct((n_dst * DB, n_src * SB), F32),
            jax.ShapeDtypeStruct((n_dst * DB, width), F32),
        ],
        compiler_params=pltpu.CompilerParams(
            dimension_semantics=("arbitrary",), vmem_limit_bytes=56 << 20
        ),
        cost_estimate=pl.CostEstimate(flops=10**11, bytes_accessed=7 * 10**7, transcendentals=0),
        name="build_adjacency",
    )(k_first, k_last, keys, low.reshape(n_chunks, 1, CH), w.reshape(n_chunks, 1, CH), table)


def multiply(a, table):
    rows, depth = a.shape
    width = table.shape[1]
    return pl.pallas_call(
        block_product,
        grid=(rows // DB,),
        in_specs=[
            pl.BlockSpec((DB, depth), lambda i: (i, 0)),
            pl.BlockSpec((depth, width), lambda i: (0, 0), pipeline_mode=pl.Buffered(1)),
        ],
        out_specs=pl.BlockSpec((DB, width), lambda i: (i, 0)),
        out_shape=jax.ShapeDtypeStruct((rows, width), F32),
        compiler_params=pltpu.CompilerParams(dimension_semantics=("arbitrary",), vmem_limit_bytes=56 << 20),
        cost_estimate=pl.CostEstimate(flops=3 * 2 * rows * depth * width, bytes_accessed=4 * rows * depth, transcendentals=0),
        name="multiply_adjacency",
    )(a, table)


def solution(mesh):
    rows_axes = ("data", "graph")
    n_graph = mesh.shape["graph"]
    swap = [(0, 1), (1, 0)]

    def device_program(x_loc, dst, src, valid, w, send_idx, send_valid, hub_ids, w_first, w_second, b_first, b_second):
        verts = x_loc.shape[0]
        hubs = hub_ids.shape[0]
        own_hubs = hubs // n_graph
        halo = send_idx.shape[1]
        width = b_first.shape[0]
        me = lax.axis_index("graph")
        col = lax.axis_index("feat")
        n_dst = (verts + hubs) // DB
        n_src = (verts + n_graph * halo + hubs) // SB

        def columns_of(weight):
            mine = lax.dynamic_slice_in_dim(weight, col * width, width, 1)
            theirs = lax.dynamic_slice_in_dim(weight, (1 - col) * width, width, 1)
            return mine, lax.ppermute(theirs, "feat", swap)

        w1_mine, w1_other = columns_of(w_first)
        w2_mine, w2_other = columns_of(w_second)

        edges = dst.shape[0]
        padded = -(-max(edges, 131072) // CH) * CH
        bucket = lax.shift_right_logical(dst, 7) * n_src + lax.shift_right_logical(src, 8)
        key = jnp.pad(jnp.where(valid > 0, bucket, n_dst * n_src), (0, padded - edges), constant_values=n_dst * n_src)
        low = jnp.pad((dst & (DB - 1)) * SB + (src & (SB - 1)), (0, padded - edges))
        key, low, w_sorted = lax.sort((key, low, jnp.pad(w, (0, padded - edges))), num_keys=1, is_stable=False)

        owner = hub_ids // verts
        ids = jnp.arange(hubs)
        earlier = (owner[None, :] == owner[:, None]) & (ids[None, :] < ids[:, None])
        place = owner * own_hubs + jnp.sum(earlier.astype(jnp.int32), axis=1)
        hub_hot = place[:, None] == ids[None, :]
        slot_ids = me * own_hubs + jnp.arange(own_hubs)
        my_rows = jnp.sum(jnp.where(place[None, :] == slot_ids[:, None], hub_ids[None, :], 0), axis=1) - me * verts

        wanted = jnp.where(send_valid > 0, send_idx, -1)
        wanted = jnp.concatenate([wanted, jnp.broadcast_to(my_rows[None, :], (n_graph, own_hubs))], axis=1)
        wanted = wanted.reshape(-1)
        send_hot = (wanted[:, None] == jnp.arange(verts)[None, :]).astype(BF)
        hub_hot_bf = hub_hot.astype(BF)
        hub_hot_t = hub_hot.T.astype(F32)

        def table_of(mine, weight_mine, weight_other):
            other = lax.ppermute(mine, "feat", swap)
            z = jnp.dot(mine, weight_mine, preferred_element_type=F32)
            z = (z + jnp.dot(other, weight_other, preferred_element_type=F32)).astype(BF)
            out = jnp.dot(send_hot, z, preferred_element_type=F32).astype(BF)
            got = lax.all_to_all(out.reshape(n_graph, halo + own_hubs, width), "graph", 0, 0, tiled=True)
            hub_rows = got[:, halo:].reshape(hubs, width)
            hub_rows = jnp.dot(hub_hot_bf, hub_rows, preferred_element_type=F32).astype(BF)
            return jnp.concatenate([z, got[:, :halo].reshape(n_graph * halo, width), hub_rows], axis=0)

        def finish(sums, bias):
            parts = jnp.dot(hub_hot_t, sums[verts:], precision=lax.Precision.HIGHEST, preferred_element_type=F32)
            got = lax.all_to_all(parts.reshape(n_graph, own_hubs, width), "graph", 0, 0, tiled=True)
            return sums[:verts].at[my_rows].add(jnp.sum(got, axis=0)) + bias

        table = table_of(x_loc, w1_mine, w1_other)
        adjacency, sums = build_and_multiply(key, low, w_sorted, table, n_dst)
        hidden = jnp.maximum(finish(sums, b_first), 0.0).astype(BF)
        table = table_of(hidden, w2_mine, w2_other)
        return finish(multiply(adjacency, table), b_second)

    edge = P(rows_axes)
    send = P(rows_axes, None)
    in_specs = (P(rows_axes, "feat"), edge, edge, edge, edge, send, send, P("data"), P("feat", None), P("feat", None), P("feat"), P("feat"))
    return jax.shard_map(device_program, mesh=mesh, in_specs=in_specs, out_specs=P(rows_axes, "feat"), check_vma=False)
```

```python
import functools

import jax
import jax.numpy as jnp
from jax import lax
from jax.experimental import pallas as pl
from jax.experimental.pallas import tpu as pltpu
from jax.sharding import PartitionSpec as P


DB = 128
SB = 256
CH = 256
LANES = 128
UNROLL = 8
BF = jnp.bfloat16
F32 = jnp.float32
VMEM_LIMIT = 56 << 20


def over(a, n):
    return lax.shift_right_arithmetic(a, n.bit_length() - 1)


def split3(a):
    hi = a.astype(BF)
    rest = a - hi.astype(F32)
    mid = rest.astype(BF)
    low = (rest - mid.astype(F32)).astype(BF)
    return hi, mid, low


def product(load, table_ref):
    depth, _ = table_ref.shape
    total = None
    for k in range(0, depth, SB):
        pieces = jnp.concatenate(split3(load(k)), axis=0)
        part = jnp.dot(pieces, table_ref[k : k + SB, :], preferred_element_type=F32)
        total = part if total is None else total + part
    rows = total.shape[0] // 3
    return total[:rows] + total[rows : 2 * rows] + total[2 * rows :]


def store_halves(y, mine_ref, other_ref):
    width = mine_ref.shape[1]
    mine_ref[...] = y[:, :width]
    other_ref[...] = y[:, width:]


def build_kernel(n_src, first_block, kf_ref, kl_ref, begin_ref, key_ref, low_ref, w_ref, table_ref, a_ref, mine_ref, other_ref, state_ref):
    step = pl.program_id(0)
    n_chunks = key_ref.shape[0]
    per = CH // LANES

    @pl.when(step == 0)
    def _():
        state_ref[0] = begin_ref[0]
        state_ref[1] = begin_ref[1]

    first = (first_block + step) * n_src
    limit = first + n_src
    a_ref[...] = jnp.zeros_like(a_ref)

    def body(carry):
        chunk, bucket = carry
        for _ in range(UNROLL):
            live = bucket < limit
            here = jnp.minimum(chunk, n_chunks - 1)
            lows = low_ref[here]
            match = key_ref[here] == jnp.where(live, bucket, -1)
            d_low = jnp.where(match, lax.shift_right_logical(lows, 8), -1)
            s_low = lows & (SB - 1)
            d_mask = lax.broadcasted_iota(jnp.int32, (DB, CH), 0) == d_low
            pieces = [jnp.where(d_mask, piece.astype(F32), 0.0).astype(BF) for piece in split3(w_ref[here])]
            s_hot = jnp.where(lax.broadcasted_iota(jnp.int32, (SB, CH), 0) == s_low, 1.0, 0.0).astype(BF)
            got = lax.dot_general(
                jnp.concatenate(pieces, axis=0), s_hot, (((1,), (1,)), ((), ())), preferred_element_type=F32
            )
            got = got[:DB] + got[DB : 2 * DB] + got[2 * DB :]
            column = pl.multiple_of(jnp.clip(bucket - first, 0, n_src - 1) * SB, SB)
            a_ref[:, pl.ds(column, SB)] += got
            done = bucket >= kl_ref[here * per + per - 1]
            next_chunk = chunk + jnp.where(done, 1, 0)
            next_bucket = jnp.where(done, kf_ref[next_chunk * per], bucket + 1)
            chunk = jnp.where(live, next_chunk, chunk)
            bucket = jnp.where(live, next_bucket, bucket)
        return chunk, bucket

    chunk, bucket = lax.while_loop(lambda c: c[1] < limit, body, (state_ref[0], state_ref[1]))
    state_ref[0] = chunk
    state_ref[1] = bucket
    store_halves(product(lambda k: a_ref[:, k : k + SB], table_ref), mine_ref, other_ref)


def build_and_multiply(edges, begin, table, first_block, n_blocks):
    k_first, k_last, keys, low, w = edges
    depth, full = table.shape
    n_src = depth // SB
    n_chunks = keys.shape[0]
    whole = lambda *shape: pl.BlockSpec(shape, lambda i, *_: (0,) * len(shape), pipeline_mode=pl.Buffered(1))
    rows = n_blocks * DB
    half = pl.BlockSpec((DB, full // 2), lambda i, *_: (i, 0))
    return pl.pallas_call(
        functools.partial(build_kernel, n_src, first_block),
        grid_spec=pltpu.PrefetchScalarGridSpec(
            num_scalar_prefetch=3,
            grid=(n_blocks,),
            in_specs=[whole(n_chunks, 1, CH)] * 3 + [whole(depth, full)],
            out_specs=[
                pl.BlockSpec((DB, depth), lambda i, *_: (i, 0)),
                half,
                half,
                pl.BlockSpec(memory_space=pltpu.SMEM),
            ],
        ),
        out_shape=[
            jax.ShapeDtypeStruct((rows, depth), F32),
            jax.ShapeDtypeStruct((rows, full // 2), F32),
            jax.ShapeDtypeStruct((rows, full // 2), F32),
            jax.ShapeDtypeStruct((2,), jnp.int32),
        ],
        compiler_params=pltpu.CompilerParams(dimension_semantics=("arbitrary",), vmem_limit_bytes=VMEM_LIMIT),
        cost_estimate=pl.CostEstimate(flops=n_blocks * 2 * 10**9, bytes_accessed=8 * rows * depth, transcendentals=0),
        name="build_adjacency",
    )(k_first, k_last, begin, keys, low, w, table)


def multiply_kernel(*refs):
    *a_refs, table_ref, mine_ref, other_ref = refs
    cols = a_refs[0].shape[1]
    load = lambda k: a_refs[k // cols][:, k % cols : k % cols + SB]
    store_halves(product(load, table_ref), mine_ref, other_ref)


def multiply(a, table):
    rows, depth = a.shape
    full = table.shape[1]
    cols = 2 * SB
    tall = 2 * DB
    half = pl.BlockSpec((tall, full // 2), lambda i: (i, 0))
    strip = lambda j: pl.BlockSpec((tall, cols), lambda i: (i, j))
    n_strips = depth // cols
    return pl.pallas_call(
        multiply_kernel,
        grid=(rows // tall,),
        in_specs=[strip(j) for j in range(n_strips)]
        + [pl.BlockSpec((depth, full), lambda i: (0, 0), pipeline_mode=pl.Buffered(1))],
        out_specs=[half, half],
        out_shape=[jax.ShapeDtypeStruct((rows, full // 2), F32)] * 2,
        compiler_params=pltpu.CompilerParams(dimension_semantics=("arbitrary",), vmem_limit_bytes=VMEM_LIMIT),
        cost_estimate=pl.CostEstimate(flops=6 * rows * depth * full, bytes_accessed=4 * rows * depth, transcendentals=0),
        name="multiply_adjacency",
    )(*[a] * n_strips, table)


def solution(mesh):
    rows_axes = ("data", "graph")
    n_graph = mesh.shape["graph"]
    swap = [(0, 1), (1, 0)]

    def device_program(x_loc, dst, src, valid, w, send_idx, send_valid, hub_ids, w_first, w_second, b_first, b_second):
        verts = x_loc.shape[0]
        hubs = hub_ids.shape[0]
        own_hubs = hubs // n_graph
        halo = send_idx.shape[1]
        width = b_first.shape[0]
        me = lax.axis_index("graph")
        col = lax.axis_index("feat")
        v_half, s_half, k_half = verts // 2, halo // 2, hubs // 2
        depth = v_half + n_graph * s_half + k_half
        n_src = depth // SB
        hub_blocks, local_blocks = hubs // DB, verts // DB
        none = (hub_blocks + local_blocks) * n_src

        def columns_of(weight):
            mine = lax.dynamic_slice_in_dim(weight, col * width, width, 1)
            theirs = lax.dynamic_slice_in_dim(weight, (1 - col) * width, width, 1)
            weight = jnp.concatenate([mine, theirs], axis=1)
            other = lax.ppermute(weight, "feat", swap)
            return weight, jnp.concatenate([other[:, width:], other[:, :width]], axis=1)

        w1 = columns_of(w_first)
        w2 = columns_of(w_second)

        in_halo = src - verts
        in_hub = in_halo - n_graph * halo
        is_own, is_halo = in_halo < 0, in_hub < 0
        half = jnp.where(is_own, over(src, v_half), jnp.where(is_halo, over(in_halo & (halo - 1), s_half), over(in_hub, k_half)))
        row = jnp.where(
            is_own,
            src & (v_half - 1),
            jnp.where(
                is_halo,
                v_half + over(in_halo, halo) * s_half + (in_halo & (s_half - 1)),
                v_half + n_graph * s_half + (in_hub & (k_half - 1)),
            ),
        )
        target = jnp.where(dst >= verts, dst - verts, dst + hubs)
        bucket = lax.shift_right_logical(target, 7) * n_src + lax.shift_right_logical(row, 8)
        n_edges = dst.shape[0]
        padded = -(-max(n_edges, 131072) // CH) * CH
        fill = (0, padded - n_edges)
        key = jnp.pad(jnp.where((valid > 0) & (half == col), bucket, none), fill, constant_values=none)
        low = jnp.pad((target & (DB - 1)) * SB + (row & (SB - 1)), fill)
        key, low, w_sorted = lax.sort((key, low, jnp.pad(w, fill)), num_keys=1, is_stable=False)
        key_rows = key.reshape(-1, LANES)
        end = jnp.full((8,), none, jnp.int32)
        k_first = jnp.concatenate([jnp.min(key_rows, axis=1), end])
        k_last = jnp.concatenate([jnp.max(key_rows, axis=1), end])
        chunks = lambda a: a.reshape(padded // CH, 1, CH)
        edges = (k_first, k_last, chunks(key), chunks(low), chunks(w_sorted))

        owner = over(hub_ids, verts)
        ids = jnp.arange(hubs)
        earlier = (owner[None, :] == owner[:, None]) & (ids[None, :] < ids[:, None])
        place = owner * own_hubs + jnp.sum(earlier.astype(jnp.int32), axis=1)
        place_half = lax.dynamic_slice_in_dim(place, col * k_half, k_half)
        hub_hot = (place_half[:, None] == ids[None, :]).astype(BF)
        hub_hot_t = (place[None, :] == ids[:, None]).astype(BF)
        slot_ids = me * own_hubs + jnp.arange(own_hubs)
        my_rows = jnp.sum(jnp.where(place[None, :] == slot_ids[:, None], hub_ids[None, :], 0), axis=1) - me * verts

        wanted = jnp.where(send_valid > 0, send_idx, -1)
        wanted = lax.dynamic_slice_in_dim(wanted, col * s_half, s_half, 1)
        wanted = jnp.concatenate([wanted, jnp.broadcast_to(my_rows[None, :], (n_graph, own_hubs))], axis=1)
        wanted = wanted.reshape(-1)
        send_hot = (wanted[:, None] == jnp.arange(verts)[None, :]).astype(BF)

        def table_of(mine, weights):
            other = lax.ppermute(mine, "feat", swap)
            z = jnp.dot(mine, weights[0], preferred_element_type=F32)
            z = (z + jnp.dot(other, weights[1], preferred_element_type=F32)).astype(BF)
            out = jnp.dot(send_hot, z, preferred_element_type=F32).astype(BF)
            got = lax.all_to_all(out.reshape(n_graph, s_half + own_hubs, 2 * width), "graph", 0, 0, tiled=True)
            hub_rows = got[:, s_half:].reshape(hubs, 2 * width)
            hub_rows = jnp.dot(hub_hot, hub_rows, preferred_element_type=F32).astype(BF)
            own = lax.dynamic_slice_in_dim(z, col * v_half, v_half)
            return jnp.concatenate([own, got[:, :s_half].reshape(n_graph * s_half, 2 * width), hub_rows], axis=0)

        def hub_parts(mine, other):
            sums = mine + lax.ppermute(other, "feat", swap)
            hi = lax.reduce_precision(sums, 8, 7)
            mid = lax.reduce_precision(sums - hi, 8, 7)
            pieces = jnp.concatenate([hi.astype(BF), mid.astype(BF), ((sums - hi) - mid).astype(BF)], axis=1)
            got = jnp.dot(hub_hot_t, pieces, preferred_element_type=F32)
            return got[:, :width] + got[:, width : 2 * width] + got[:, 2 * width :]

        def hub_total(parts):
            got = lax.all_to_all(parts.reshape(n_graph, own_hubs, width), "graph", 0, 0, tiled=True)
            return jnp.sum(got, axis=0)

        def finish(mine, other, total, bias):
            return (mine + lax.ppermute(other, "feat", swap) + bias).at[my_rows].add(total)

        table = table_of(x_loc, w1)
        begin = jnp.stack([jnp.int32(0), k_first[0]])
        a_hub, mine, other, state = build_and_multiply(edges, begin, table, 0, hub_blocks)
        parts, state = lax.optimization_barrier((hub_parts(mine, other), state))
        total = hub_total(parts)
        a_local, mine, other, _ = build_and_multiply(edges, state, table, hub_blocks, local_blocks)
        hidden = jnp.maximum(finish(mine, other, total, b_first), 0.0).astype(BF)

        table = table_of(hidden, w2)
        parts, table_local = lax.optimization_barrier((hub_parts(*multiply(a_hub, table)), table))
        total = hub_total(parts)
        mine, other = multiply(a_local, table_local)
        return finish(mine, other, total, b_second)

    edge = P(rows_axes)
    send = P(rows_axes, None)
    in_specs = (P(rows_axes, "feat"), edge, edge, edge, edge, send, send, P("data"), P("feat", None), P("feat", None), P("feat"), P("feat"))
    return jax.shard_map(device_program, mesh=mesh, in_specs=in_specs, out_specs=P(rows_axes, "feat"), check_vma=False)
```

```python
import functools

import jax
import jax.numpy as jnp
from jax import lax
from jax.experimental import pallas as pl
from jax.experimental.pallas import tpu as pltpu
from jax.sharding import PartitionSpec as P


DB = 128
SB = 256
CH = 256
LANES = 128
UNROLL = 8
BF = jnp.bfloat16
F32 = jnp.float32
VMEM_LIMIT = 60 << 20


def over(a, n):
    return lax.shift_right_arithmetic(a, n.bit_length() - 1)


def split3(a):
    hi = a.astype(BF)
    rest = a - hi.astype(F32)
    mid = rest.astype(BF)
    low = (rest - mid.astype(F32)).astype(BF)
    return hi, mid, low


def product(a_ref, start, table_ref):
    depth, _ = table_ref.shape
    total = None
    for k in range(0, depth, SB):
        pieces = jnp.concatenate(split3(a_ref[pl.ds(start, DB), k : k + SB]), axis=0)
        part = jnp.dot(pieces, table_ref[k : k + SB, :], preferred_element_type=F32)
        total = part if total is None else total + part
    return total[:DB] + total[DB : 2 * DB] + total[2 * DB :]


def write_product(a_ref, i, table_ref, mine_ref, other_ref):
    width = mine_ref.shape[1]
    start = pl.multiple_of(i * DB, DB)
    y = product(a_ref, start, table_ref)
    mine_ref[pl.ds(start, DB), :] = y[:, :width]
    other_ref[pl.ds(start, DB), :] = y[:, width:]


def block_copy(src, dst, i, sem):
    rows = pl.ds(pl.multiple_of(i * DB, DB), DB)
    return pltpu.make_async_copy(src.at[rows, :], dst.at[rows, :], sem.at[i])


def multiply_kernel(a_hbm, table_ref, mine_ref, other_ref, a_ref, sem):
    n_blocks = a_ref.shape[0] // DB

    @pl.loop(0, n_blocks)
    def _(i):
        block_copy(a_hbm, a_ref, i, sem).start()

    @pl.loop(0, n_blocks)
    def _(i):
        block_copy(a_hbm, a_ref, i, sem).wait()
        write_product(a_ref, i, table_ref, mine_ref, other_ref)


def build_kernel(first_block, kf_ref, kl_ref, begin_ref, key_ref, low_ref, w_ref, table_ref, a_hbm, mine_ref, other_ref, state_ref, a_ref, sem):
    n_src = a_ref.shape[1] // SB
    n_rows = key_ref.shape[0]
    n_blocks = a_ref.shape[0] // DB
    first = first_block * n_src
    limit = first + n_blocks * n_src

    @pl.loop(0, n_blocks)
    def _(i):
        a_ref[pl.ds(pl.multiple_of(i * DB, DB), DB), :] = jnp.zeros((DB, a_ref.shape[1]), F32)

    def pair(ref, at):
        return jnp.concatenate([ref[at], ref[at + 1]], axis=1)

    def body(carry):
        at, bucket = carry
        for _ in range(UNROLL):
            live = bucket < limit
            here = jnp.minimum(at, n_rows - 2)
            lows = pair(low_ref, here)
            match = pair(key_ref, here) == jnp.where(live, bucket, -1)
            d_low = jnp.where(match, lax.shift_right_logical(lows, 8), -1)
            s_low = lows & (SB - 1)
            d_mask = lax.broadcasted_iota(jnp.int32, (DB, CH), 0) == d_low
            pieces = [jnp.where(d_mask, piece.astype(F32), 0.0).astype(BF) for piece in split3(pair(w_ref, here))]
            s_hot = jnp.where(lax.broadcasted_iota(jnp.int32, (SB, CH), 0) == s_low, 1.0, 0.0).astype(BF)
            got = lax.dot_general(
                jnp.concatenate(pieces, axis=0), s_hot, (((1,), (1,)), ((), ())), preferred_element_type=F32
            )
            got = got[:DB] + got[DB : 2 * DB] + got[2 * DB :]
            place = jnp.clip(bucket - first, 0, n_blocks * n_src - 1)
            block = place // n_src
            column = pl.multiple_of((place - block * n_src) * SB, SB)
            a_ref[pl.ds(pl.multiple_of(block * DB, DB), DB), pl.ds(column, SB)] += got
            more = kl_ref[here + 1] == bucket
            next_at = here + jnp.where(more, 2, jnp.where(kl_ref[here] <= bucket, 1, 0))
            next_bucket = jnp.maximum(kf_ref[next_at], jnp.where(more, bucket, bucket + 1))
            at = jnp.where(live, next_at, at)
            bucket = jnp.where(live, next_bucket, bucket)
        return at, bucket

    at, bucket = lax.while_loop(lambda c: c[1] < limit, body, (begin_ref[0], begin_ref[1]))
    state_ref[0] = at
    state_ref[1] = bucket

    @pl.loop(0, n_blocks)
    def _(i):
        block_copy(a_ref, a_hbm, i, sem).start()

    @pl.loop(0, n_blocks)
    def _(i):
        write_product(a_ref, i, table_ref, mine_ref, other_ref)

    @pl.loop(0, n_blocks)
    def _(i):
        block_copy(a_ref, a_hbm, i, sem).wait()


HBM_SPEC = pl.BlockSpec(memory_space=pltpu.HBM)
SMEM_SPEC = pl.BlockSpec(memory_space=pltpu.SMEM)
VMEM_SPEC = pl.BlockSpec(memory_space=pltpu.VMEM)


def build_and_multiply(edges, begin, table, first_block, n_blocks):
    k_first, k_last, keys, low, w = edges
    depth, full = table.shape
    rows = n_blocks * DB
    return pl.pallas_call(
        functools.partial(build_kernel, first_block),
        in_specs=[SMEM_SPEC] * 3 + [VMEM_SPEC] * 4,
        out_specs=[HBM_SPEC, VMEM_SPEC, VMEM_SPEC, SMEM_SPEC],
        scratch_shapes=[pltpu.VMEM((rows, depth), F32), pltpu.SemaphoreType.DMA((n_blocks,))],
        out_shape=[
            jax.ShapeDtypeStruct((rows, depth), F32),
            jax.ShapeDtypeStruct((rows, full // 2), F32),
            jax.ShapeDtypeStruct((rows, full // 2), F32),
            jax.ShapeDtypeStruct((2,), jnp.int32),
        ],
        compiler_params=pltpu.CompilerParams(vmem_limit_bytes=VMEM_LIMIT),
        cost_estimate=pl.CostEstimate(flops=n_blocks * 2 * 10**9, bytes_accessed=10**7, transcendentals=0),
        name="build_adjacency",
    )(k_first, k_last, begin, keys, low, w, table)


def multiply(a, table):
    rows, depth = a.shape
    full = table.shape[1]
    return pl.pallas_call(
        multiply_kernel,
        in_specs=[HBM_SPEC, VMEM_SPEC],
        out_specs=[VMEM_SPEC] * 2,
        scratch_shapes=[pltpu.VMEM((rows, depth), F32), pltpu.SemaphoreType.DMA((rows // DB,))],
        out_shape=[jax.ShapeDtypeStruct((rows, full // 2), F32)] * 2,
        compiler_params=pltpu.CompilerParams(vmem_limit_bytes=VMEM_LIMIT),
        cost_estimate=pl.CostEstimate(flops=6 * rows * depth * full, bytes_accessed=10**7, transcendentals=0),
        name="multiply_adjacency",
    )(a, table)


def solution(mesh):
    rows_axes = ("data", "graph")
    n_graph = mesh.shape["graph"]
    swap = [(0, 1), (1, 0)]

    def device_program(x_loc, dst, src, valid, w, send_idx, send_valid, hub_ids, w_first, w_second, b_first, b_second):
        verts = x_loc.shape[0]
        hubs = hub_ids.shape[0]
        own_hubs = hubs // n_graph
        halo = send_idx.shape[1]
        width = b_first.shape[0]
        me = lax.axis_index("graph")
        col = lax.axis_index("feat")
        v_half, s_half, k_half = verts // 2, halo // 2, hubs // 2
        depth = v_half + n_graph * s_half + k_half
        n_src = depth // SB
        hub_blocks, local_blocks = hubs // DB, verts // DB
        none = (hub_blocks + local_blocks) * n_src

        def columns_of(weight):
            mine = lax.dynamic_slice_in_dim(weight, col * width, width, 1)
            theirs = lax.dynamic_slice_in_dim(weight, (1 - col) * width, width, 1)
            weight = jnp.concatenate([mine, theirs], axis=1)
            other = lax.ppermute(weight, "feat", swap)
            return weight, jnp.concatenate([other[:, width:], other[:, :width]], axis=1)

        w1 = columns_of(w_first)
        w2 = columns_of(w_second)

        in_halo = src - verts
        in_hub = in_halo - n_graph * halo
        is_own, is_halo = in_halo < 0, in_hub < 0
        half = jnp.where(is_own, over(src, v_half), jnp.where(is_halo, over(in_halo & (halo - 1), s_half), over(in_hub, k_half)))
        row = jnp.where(
            is_own,
            src & (v_half - 1),
            jnp.where(
                is_halo,
                v_half + over(in_halo, halo) * s_half + (in_halo & (s_half - 1)),
                v_half + n_graph * s_half + (in_hub & (k_half - 1)),
            ),
        )
        target = jnp.where(dst >= verts, dst - verts, dst + hubs)
        bucket = lax.shift_right_logical(target, 7) * n_src + lax.shift_right_logical(row, 8)
        n_edges = dst.shape[0]
        padded = -(-max(n_edges + 2 * CH, 131072) // CH) * CH
        fill = (0, padded - n_edges)
        key = jnp.pad(jnp.where((valid > 0) & (half == col), bucket, none), fill, constant_values=none)
        low = jnp.pad((target & (DB - 1)) * SB + (row & (SB - 1)), fill)
        key, low, w_sorted = lax.sort((key, low, jnp.pad(w, fill)), num_keys=1, is_stable=False)
        key_rows = key.reshape(-1, LANES)
        end = jnp.full((8,), none, jnp.int32)
        k_first = jnp.concatenate([jnp.min(key_rows, axis=1), end])
        k_last = jnp.concatenate([jnp.max(key_rows, axis=1), end])
        rows_of = lambda a: a.reshape(-1, 1, LANES)
        edges = (k_first, k_last, rows_of(key), rows_of(low), rows_of(w_sorted))

        owner = over(hub_ids, verts)
        ids = jnp.arange(hubs)
        earlier = (owner[None, :] == owner[:, None]) & (ids[None, :] < ids[:, None])
        place = owner * own_hubs + jnp.sum(earlier.astype(jnp.int32), axis=1)
        place_half = lax.dynamic_slice_in_dim(place, col * k_half, k_half)
        hub_hot = (place_half[:, None] == ids[None, :]).astype(BF)
        hub_hot_t = (place[None, :] == ids[:, None]).astype(BF)
        slot_ids = me * own_hubs + jnp.arange(own_hubs)
        my_rows = jnp.sum(jnp.where(place[None, :] == slot_ids[:, None], hub_ids[None, :], 0), axis=1) - me * verts

        wanted = jnp.where(send_valid > 0, send_idx, -1)
        wanted = lax.dynamic_slice_in_dim(wanted, col * s_half, s_half, 1)
        wanted = jnp.concatenate([wanted, jnp.broadcast_to(my_rows[None, :], (n_graph, own_hubs))], axis=1)
        wanted = wanted.reshape(-1)
        send_hot = (wanted[:, None] == jnp.arange(verts)[None, :]).astype(BF)

        def table_of(mine, weights):
            other = lax.ppermute(mine, "feat", swap)
            z = jnp.dot(mine, weights[0], preferred_element_type=F32)
            z = (z + jnp.dot(other, weights[1], preferred_element_type=F32)).astype(BF)
            out = jnp.dot(send_hot, z, preferred_element_type=F32).astype(BF)
            got = lax.all_to_all(out.reshape(n_graph, s_half + own_hubs, 2 * width), "graph", 0, 0, tiled=True)
            hub_rows = got[:, s_half:].reshape(hubs, 2 * width)
            hub_rows = jnp.dot(hub_hot, hub_rows, preferred_element_type=F32).astype(BF)
            own = lax.dynamic_slice_in_dim(z, col * v_half, v_half)
            return jnp.concatenate([own, got[:, :s_half].reshape(n_graph * s_half, 2 * width), hub_rows], axis=0)

        def hub_parts(mine, other):
            sums = mine + lax.ppermute(other, "feat", swap)
            hi = lax.reduce_precision(sums, 8, 7)
            mid = lax.reduce_precision(sums - hi, 8, 7)
            pieces = jnp.concatenate([hi.astype(BF), mid.astype(BF), ((sums - hi) - mid).astype(BF)], axis=1)
            got = jnp.dot(hub_hot_t, pieces, preferred_element_type=F32)
            return got[:, :width] + got[:, width : 2 * width] + got[:, 2 * width :]

        def hub_total(parts):
            got = lax.all_to_all(parts.reshape(n_graph, own_hubs, width), "graph", 0, 0, tiled=True)
            return jnp.sum(got, axis=0)

        def finish(mine, other, total, bias):
            return (mine + lax.ppermute(other, "feat", swap) + bias).at[my_rows].add(total)

        table = table_of(x_loc, w1)
        begin = jnp.stack([jnp.int32(0), k_first[0]])
        a_hub, mine, other, state = build_and_multiply(edges, begin, table, 0, hub_blocks)
        parts, state = lax.optimization_barrier((hub_parts(mine, other), state))
        total = hub_total(parts)
        a_local, mine, other, _ = build_and_multiply(edges, state, table, hub_blocks, local_blocks)
        hidden = jnp.maximum(finish(mine, other, total, b_first), 0.0).astype(BF)

        table = table_of(hidden, w2)
        parts, table_local = lax.optimization_barrier((hub_parts(*multiply(a_hub, table)), table))
        total = hub_total(parts)
        mine, other = multiply(a_local, table_local)
        return finish(mine, other, total, b_second)

    edge = P(rows_axes)
    send = P(rows_axes, None)
    in_specs = (P(rows_axes, "feat"), edge, edge, edge, edge, send, send, P("data"), P("feat", None), P("feat", None), P("feat"), P("feat"))
    return jax.shard_map(device_program, mesh=mesh, in_specs=in_specs, out_specs=P(rows_axes, "feat"), check_vma=False)
```

```python
import functools

import jax
import jax.numpy as jnp
from jax import lax
from jax.experimental import pallas as pl
from jax.experimental.pallas import tpu as pltpu
from jax.sharding import PartitionSpec as P

DB = 128
SB = 256
CH = 256
LANES = 128
UNROLL = 8
BF = jnp.bfloat16
F32 = jnp.float32
VMEM_LIMIT = 60 << 20
FRONT_LIMIT = 24 << 20


def over(a, n):
    return lax.shift_right_arithmetic(a, n.bit_length() - 1)


def split3(a):
    hi = a.astype(BF)
    rest = a - hi.astype(F32)
    mid = rest.astype(BF)
    low = (rest - mid.astype(F32)).astype(BF)
    return hi, mid, low


def product(a_ref, start, table_ref):
    depth, width = table_ref.shape
    total = None
    for k in range(0, depth, SB):
        pieces = jnp.concatenate(split3(a_ref[pl.ds(start, DB), k : k + SB]), axis=0)
        part = jnp.dot(pieces, table_ref[k : k + SB, :], preferred_element_type=F32)
        total = part if total is None else total + part
    return total[:DB] + total[DB : 2 * DB] + total[2 * DB :]


def write_product(a_ref, i, table_ref, mine_ref, other_ref):
    width = mine_ref.shape[1]
    start = pl.multiple_of(i * DB, DB)
    y = product(a_ref, start, table_ref)
    mine_ref[pl.ds(start, DB), :] = y[:, :width]
    other_ref[pl.ds(start, DB), :] = y[:, width:]


def block_copy(src, dst, i, sem):
    rows = pl.ds(pl.multiple_of(i * DB, DB), DB)
    return pltpu.make_async_copy(src.at[rows, :], dst.at[rows, :], sem.at[i])


def build_kernel(kf_ref, kl_ref, key_ref, low_ref, w_ref, table_ref, a_hbm, mine_ref, other_ref, a_ref, sem):
    n_src = a_ref.shape[1] // SB
    n_rows = key_ref.shape[0]
    n_blocks = a_ref.shape[0] // DB
    limit = n_blocks * n_src

    @pl.loop(0, n_blocks)
    def _(i):
        a_ref[pl.ds(pl.multiple_of(i * DB, DB), DB), :] = jnp.zeros((DB, a_ref.shape[1]), F32)

    def pair(ref, at):
        return jnp.concatenate([ref[at], ref[at + 1]], axis=1)

    def body(carry):
        at, bucket = carry
        for _ in range(UNROLL):
            live = bucket < limit
            here = jnp.minimum(at, n_rows - 2)
            lows = pair(low_ref, here)
            match = pair(key_ref, here) == jnp.where(live, bucket, -1)
            d_low = jnp.where(match, lax.shift_right_logical(lows, 8), -1)
            s_low = lows & (SB - 1)
            d_mask = lax.broadcasted_iota(jnp.int32, (DB, CH), 0) == d_low
            pieces = [jnp.where(d_mask, piece.astype(F32), 0.0).astype(BF) for piece in split3(pair(w_ref, here))]
            s_hot = jnp.where(lax.broadcasted_iota(jnp.int32, (SB, CH), 0) == s_low, 1.0, 0.0).astype(BF)
            got = lax.dot_general(
                jnp.concatenate(pieces, axis=0), s_hot, (((1,), (1,)), ((), ())), preferred_element_type=F32
            )
            got = got[:DB] + got[DB : 2 * DB] + got[2 * DB :]
            place = jnp.minimum(bucket, limit - 1)
            block = place // n_src
            column = pl.multiple_of((place - block * n_src) * SB, SB)
            a_ref[pl.ds(pl.multiple_of(block * DB, DB), DB), pl.ds(column, SB)] += got
            more = kl_ref[here + 1] == bucket
            next_at = here + jnp.where(more, 2, jnp.where(kl_ref[here] <= bucket, 1, 0))
            next_bucket = jnp.maximum(kf_ref[next_at], jnp.where(more, bucket, bucket + 1))
            at = jnp.where(live, next_at, at)
            bucket = jnp.where(live, next_bucket, bucket)
        return at, bucket

    lax.while_loop(lambda c: c[1] < limit, body, (jnp.int32(0), kf_ref[0]))

    @pl.loop(0, n_blocks)
    def _(i):
        block_copy(a_ref, a_hbm, i, sem).start()

    @pl.loop(0, n_blocks)
    def _(i):
        write_product(a_ref, i, table_ref, mine_ref, other_ref)

    @pl.loop(0, n_blocks)
    def _(i):
        block_copy(a_ref, a_hbm, i, sem).wait()


HBM_SPEC = pl.BlockSpec(memory_space=pltpu.HBM)
SMEM_SPEC = pl.BlockSpec(memory_space=pltpu.SMEM)
VMEM_SPEC = pl.BlockSpec(memory_space=pltpu.VMEM)


def build_and_multiply(edges, table, n_blocks):
    depth, full = table.shape
    rows = n_blocks * DB
    return pl.pallas_call(
        build_kernel,
        in_specs=[SMEM_SPEC] * 2 + [VMEM_SPEC] * 4,
        out_specs=[HBM_SPEC, VMEM_SPEC, VMEM_SPEC],
        scratch_shapes=[pltpu.VMEM((rows, depth), F32), pltpu.SemaphoreType.DMA((n_blocks,))],
        out_shape=[
            jax.ShapeDtypeStruct((rows, depth), F32),
            jax.ShapeDtypeStruct((rows, full // 2), F32),
            jax.ShapeDtypeStruct((rows, full // 2), F32),
        ],
        compiler_params=pltpu.CompilerParams(vmem_limit_bytes=VMEM_LIMIT),
        cost_estimate=pl.CostEstimate(flops=n_blocks * 2 * 10**9, bytes_accessed=10**7, transcendentals=0),
        name="build_adjacency",
    )(*edges, table)


MESH = pl.DeviceIdType.MESH


def block(i, size):
    return pl.ds(pl.multiple_of(i * size, size), size)


def hot(condition):
    return jnp.where(condition, 1.0, 0.0).astype(BF)


def iota(shape, axis):
    return lax.broadcasted_iota(jnp.int32, shape, axis)


class Links:
    def __init__(self, n_graph, send_sem, recv_sem):
        self.n_graph, self.send_sem, self.recv_sem = n_graph, send_sem, recv_sem
        self.me = lax.axis_index("graph")
        self.col = lax.axis_index("feat")

    def peer(self, k):
        return lax.rem(self.me + k, self.n_graph)

    def copy(self, kind, src, dst, device):
        return pltpu.make_async_remote_copy(
            src_ref=src,
            dst_ref=dst,
            send_sem=self.send_sem.at[kind],
            recv_sem=self.recv_sem.at[kind],
            device_id=device,
            device_id_type=MESH,
        )

    def partner(self, kind, src, dst):
        return self.copy(kind, src, dst, {"feat": 1 - self.col})

    def announce(self, with_partner):
        barrier = pltpu.get_barrier_semaphore()

        @pl.loop(1, self.n_graph)
        def _(k):
            pl.semaphore_signal(barrier, inc=1, device_id={"graph": self.peer(k)}, device_id_type=MESH)

        if with_partner:
            pl.semaphore_signal(barrier, inc=1, device_id={"feat": 1 - self.col}, device_id_type=MESH)

    def everyone_in(self, with_partner):
        pl.semaphore_wait(pltpu.get_barrier_semaphore(), self.n_graph - 1 + int(with_partner))

    def wait(self, kind, src, dst):
        self.partner(kind, src, dst).wait()


def send_rows(z_ref, wanted_ref, my_rows_ref, out_ref, hub_out_ref):
    verts = z_ref.shape[0]

    def pick(index):
        parts = [hot(index == iota(index.shape, 1) + t * LANES) for t in range(verts // LANES)]
        rows = jnp.concatenate(parts, axis=1)
        return jnp.dot(rows, z_ref[...], preferred_element_type=F32).astype(BF)

    hub_out_ref[...] = pick(my_rows_ref[...])
    group = 2 * DB

    @pl.loop(0, out_ref.shape[0] // group)
    def _(i):
        out_ref[block(i, group), :] = pick(wanted_ref[block(i, group), :])


def start_rows(links, halo_kind, hub_kind, out_ref, hub_out_ref, table_ref, hub_in_ref, v_half):
    own_hubs = hub_out_ref.shape[0]
    s_half = out_ref.shape[0] // links.n_graph
    here = table_ref.at[pl.ds(pl.multiple_of(v_half + links.me * s_half, s_half), s_half), :]
    hub_here = hub_in_ref.at[block(links.me, own_hubs), :]

    @pl.loop(1, links.n_graph)
    def _(k):
        peer = links.peer(k)
        links.copy(halo_kind, out_ref.at[block(peer, s_half), :], here, {"graph": peer}).start()
        links.copy(hub_kind, hub_out_ref, hub_here, {"graph": peer}).start()

    here[...] = out_ref[block(links.me, s_half), :]
    hub_here[...] = hub_out_ref[...]


def finish_table(links, halo_kind, hub_kind, z_ref, out_ref, place_half_ref, table_ref, hub_in_ref, v_half):
    others = links.n_graph - 1
    s_half = out_ref.shape[0] // links.n_graph
    own_hubs = hub_in_ref.shape[0] // links.n_graph
    table_ref[0:v_half, :] = z_ref[pl.ds(pl.multiple_of(links.col * v_half, v_half), v_half), :]
    hub_part = hub_in_ref.at[0 : others * own_hubs, :]
    links.wait(hub_kind, hub_part, hub_part)
    halo_part = table_ref.at[v_half : v_half + others * s_half, :]
    links.wait(halo_kind, halo_part, halo_part)
    hubs, k_half = hub_in_ref.shape[0], place_half_ref.shape[0]
    index = place_half_ref[...]
    rows = jnp.concatenate([hot(index == iota(index.shape, 1) + t * LANES) for t in range(hubs // LANES)], axis=1)
    first = v_half + out_ref.shape[0]
    table_ref[first : first + k_half, :] = jnp.dot(rows, hub_in_ref[...], preferred_element_type=F32).astype(BF)


def front_kernel(n_graph, z_ref, wanted_ref, my_rows_ref, place_half_ref, result_ref, table_ref, out_ref, hub_out_ref, hub_in_ref, send_sem, recv_sem):
    links = Links(n_graph, send_sem, recv_sem)
    v_half = z_ref.shape[0] // 2
    links.announce(False)
    send_rows(z_ref, wanted_ref, my_rows_ref, out_ref, hub_out_ref)
    links.everyone_in(False)
    start_rows(links, 0, 1, out_ref, hub_out_ref, table_ref, hub_in_ref, v_half)
    finish_table(links, 0, 1, z_ref, out_ref, place_half_ref, table_ref, hub_in_ref, v_half)
    result_ref[...] = table_ref[...]


def first_table(n_graph, z, wanted, my_rows, place_half, depth):
    verts, full = z.shape
    own_hubs = my_rows.shape[0]
    return pl.pallas_call(
        functools.partial(front_kernel, n_graph),
        in_specs=[VMEM_SPEC] * 4,
        out_specs=VMEM_SPEC,
        out_shape=jax.ShapeDtypeStruct((depth, full), BF),
        scratch_shapes=[
            pltpu.VMEM((depth, full), BF),
            pltpu.VMEM((wanted.shape[0], full), BF),
            pltpu.VMEM((own_hubs, full), BF),
            pltpu.VMEM((n_graph * own_hubs, full), BF),
            pltpu.SemaphoreType.DMA((2,)),
            pltpu.SemaphoreType.DMA((2,)),
        ],
        compiler_params=pltpu.CompilerParams(collective_id=0, has_side_effects=True, vmem_limit_bytes=FRONT_LIMIT),
        cost_estimate=pl.CostEstimate(flops=10**10, bytes_accessed=4 * 10**6, transcendentals=0),
        name="first_table",
    )(z, wanted, my_rows, place_half)


def rest_kernel(
    n_graph, sums_mine, sums_other, a_hbm, weights_ref, bias1_ref, bias2_ref, wanted_ref, my_rows_ref, my_line_ref,
    place_half_ref, place_line_ref, result_ref,
    a_ref, hub_rx, local_rx, pieces_ref, parts_ref, total_rx, total_ref, h_ref, h_rx, z_ref, out_ref, hub_out_ref, hub_in_ref,
    table_ref, hub_mine, hub_other, local_other, hub_rx2, local_rx2, parts_ref2, total_rx2, a_sem, send_sem, recv_sem,
):
    links = Links(n_graph, send_sem, recv_sem)
    hubs, width = hub_rx.shape
    verts = result_ref.shape[0]
    own_hubs = hubs // n_graph
    v_half = verts // 2
    n_hub_blocks = hubs // DB
    n_local_blocks = verts // DB
    tall = 2 * DB

    @pl.loop(0, n_hub_blocks + n_local_blocks)
    def _(i):
        block_copy(a_hbm, a_ref, i, a_sem).start()

    links.announce(True)
    links.everyone_in(True)
    hub_rows = sums_other.at[0:hubs, :]
    local_rows = sums_other.at[hubs : hubs + verts, :]
    links.partner(0, hub_rows, hub_rx).start()
    links.partner(1, local_rows, local_rx).start()
    total_ref[...] = jnp.zeros_like(total_ref)

    def hub_exchange(kind, own, theirs, parts, arrivals):
        @pl.loop(0, hubs // tall)
        def _(i):
            rows = block(i, tall)
            pieces_ref[rows, :] = jnp.concatenate(split3(own[rows, :] + theirs[rows, :]), axis=1)

        @pl.loop(0, hubs // tall)
        def _(i):
            rows = hot(place_line_ref[...] == iota((tall, hubs), 0) + i * tall)
            got = jnp.dot(rows, pieces_ref[...], preferred_element_type=F32)
            parts[block(i, tall), :] = got[:, :width] + got[:, width : 2 * width] + got[:, 2 * width :]

        here = arrivals.at[block(links.me, own_hubs), :]

        @pl.loop(1, n_graph)
        def _(k):
            peer = links.peer(k)
            links.copy(kind, parts.at[block(peer, own_hubs), :], here, {"graph": peer}).start()

        here[...] = parts[block(links.me, own_hubs), :]

    def hub_total(kind, arrivals):
        part = arrivals.at[0 : (n_graph - 1) * own_hubs, :]
        links.wait(kind, part, part)
        total = jnp.sum(arrivals[...].reshape(n_graph, own_hubs, width), axis=0)
        total_ref[0:own_hubs, :] = jnp.concatenate(split3(total), axis=1)

    def hub_add(i):
        at = hot(my_line_ref[...] == iota((tall, LANES), 0) + i * tall)
        got = jnp.dot(at, total_ref[...], preferred_element_type=F32)
        return got[:, :width] + got[:, width : 2 * width] + got[:, 2 * width :]

    links.wait(0, hub_rows, hub_rx)
    hub_exchange(2, sums_mine, hub_rx, parts_ref, total_rx)
    links.wait(1, local_rows, local_rx)
    hub_total(2, total_rx)

    @pl.loop(0, verts // tall)
    def _(i):
        rows = block(i, tall)
        y = sums_mine[pl.ds(pl.multiple_of(hubs + i * tall, tall), tall), :] + local_rx[rows, :]
        h_ref[rows, :] = jnp.maximum(y + hub_add(i) + bias1_ref[...], 0.0).astype(BF)

    links.partner(3, h_ref, h_rx).start()
    links.wait(3, h_ref, h_rx)

    @pl.loop(0, verts // tall)
    def _(i):
        rows = block(i, tall)
        z = jnp.dot(h_ref[rows, :], weights_ref[0:width, :], preferred_element_type=F32)
        z = z + jnp.dot(h_rx[rows, :], weights_ref[width : 2 * width, :], preferred_element_type=F32)
        z_ref[rows, :] = z.astype(BF)

    send_rows(z_ref, wanted_ref, my_rows_ref, out_ref, hub_out_ref)
    start_rows(links, 4, 5, out_ref, hub_out_ref, table_ref, hub_in_ref, v_half)
    finish_table(links, 4, 5, z_ref, out_ref, place_half_ref, table_ref, hub_in_ref, v_half)

    @pl.loop(0, n_hub_blocks)
    def _(i):
        block_copy(a_hbm, a_ref, i, a_sem).wait()
        y = product(a_ref, pl.multiple_of(i * DB, DB), table_ref)
        hub_mine[block(i, DB), :] = y[:, :width]
        hub_other[block(i, DB), :] = y[:, width:]

    links.partner(6, hub_other, hub_rx2).start()
    links.wait(6, hub_other, hub_rx2)
    hub_exchange(7, hub_mine, hub_rx2, parts_ref2, total_rx2)

    @pl.loop(0, n_local_blocks)
    def _(i):
        block_copy(a_hbm, a_ref, i + n_hub_blocks, a_sem).wait()
        y = product(a_ref, pl.multiple_of(hubs + i * DB, DB), table_ref)
        rows = block(i, DB)
        result_ref[rows, :] = y[:, :width]
        local_other[rows, :] = y[:, width:]

    links.partner(8, local_other, local_rx2).start()
    hub_total(7, total_rx2)
    links.wait(8, local_other, local_rx2)

    @pl.loop(0, verts // tall)
    def _(i):
        rows = block(i, tall)
        result_ref[rows, :] = result_ref[rows, :] + local_rx2[rows, :] + hub_add(i) + bias2_ref[...]


def rest(n_graph, sums_mine, sums_other, adjacency, weights, bias1, bias2, wanted, my_rows, my_line, place_half, place_line):
    rows, depth = adjacency.shape
    hubs = place_line.shape[1]
    verts = rows - hubs
    width = bias1.shape[1]
    full = 2 * width
    own_hubs = hubs // n_graph
    half_rows = lambda n: pltpu.VMEM((n, width), F32)
    return pl.pallas_call(
        functools.partial(rest_kernel, n_graph),
        in_specs=[VMEM_SPEC, VMEM_SPEC, HBM_SPEC] + [VMEM_SPEC] * 8,
        out_specs=VMEM_SPEC,
        out_shape=jax.ShapeDtypeStruct((verts, width), F32),
        scratch_shapes=[
            pltpu.VMEM((rows, depth), F32),
            half_rows(hubs),
            half_rows(verts),
            pltpu.VMEM((hubs, 3 * width), BF),
            half_rows(hubs),
            half_rows(hubs),
            pltpu.VMEM((LANES, 3 * width), BF),
            pltpu.VMEM((verts, width), BF),
            pltpu.VMEM((verts, width), BF),
            pltpu.VMEM((verts, full), BF),
            pltpu.VMEM((wanted.shape[0], full), BF),
            pltpu.VMEM((own_hubs, full), BF),
            pltpu.VMEM((hubs, full), BF),
            pltpu.VMEM((depth, full), BF),
            half_rows(hubs),
            half_rows(hubs),
            half_rows(verts),
            half_rows(hubs),
            half_rows(verts),
            half_rows(hubs),
            half_rows(hubs),
            pltpu.SemaphoreType.DMA((rows // DB,)),
            pltpu.SemaphoreType.DMA((9,)),
            pltpu.SemaphoreType.DMA((9,)),
        ],
        compiler_params=pltpu.CompilerParams(collective_id=1, has_side_effects=True, vmem_limit_bytes=VMEM_LIMIT),
        cost_estimate=pl.CostEstimate(flops=2 * 10**10, bytes_accessed=4 * 10**7, transcendentals=0),
        name="rest",
    )(sums_mine, sums_other, adjacency, weights, bias1, bias2, wanted, my_rows, my_line, place_half, place_line)


def solution(mesh):
    rows_axes = ("data", "graph")
    n_graph = mesh.shape["graph"]
    swap = [(0, 1), (1, 0)]

    def device_program(x_loc, dst, src, valid, w, send_idx, send_valid, hub_ids, w_first, w_second, b_first, b_second):
        verts = x_loc.shape[0]
        hubs = hub_ids.shape[0]
        own_hubs = hubs // n_graph
        halo = send_idx.shape[1]
        width = b_first.shape[0]
        me = lax.axis_index("graph")
        col = lax.axis_index("feat")
        v_half, s_half, k_half = verts // 2, halo // 2, hubs // 2
        depth = v_half + n_graph * s_half + k_half
        n_src = depth // SB
        hub_blocks, local_blocks = hubs // DB, verts // DB
        none = (hub_blocks + local_blocks) * n_src

        def columns_of(weight):
            mine = lax.dynamic_slice_in_dim(weight, col * width, width, 1)
            theirs = lax.dynamic_slice_in_dim(weight, (1 - col) * width, width, 1)
            weight = jnp.concatenate([mine, theirs], axis=1)
            other = lax.ppermute(weight, "feat", swap)
            return weight, jnp.concatenate([other[:, width:], other[:, :width]], axis=1)

        w1 = columns_of(w_first)
        w2 = columns_of(w_second)

        in_halo = src - verts
        in_hub = in_halo - n_graph * halo
        is_own, is_halo = in_halo < 0, in_hub < 0
        half = jnp.where(is_own, over(src, v_half), jnp.where(is_halo, over(in_halo & (halo - 1), s_half), over(in_hub, k_half)))
        row = jnp.where(
            is_own,
            src & (v_half - 1),
            jnp.where(
                is_halo,
                v_half + over(in_halo, halo) * s_half + (in_halo & (s_half - 1)),
                v_half + n_graph * s_half + (in_hub & (k_half - 1)),
            ),
        )
        target = jnp.where(dst >= verts, dst - verts, dst + hubs)
        bucket = lax.shift_right_logical(target, 7) * n_src + lax.shift_right_logical(row, 8)
        n_edges = dst.shape[0]
        padded = -(-max(n_edges + 2 * CH, 131072) // CH) * CH
        fill = (0, padded - n_edges)
        key = jnp.pad(jnp.where((valid > 0) & (half == col), bucket, none), fill, constant_values=none)
        low = jnp.pad((target & (DB - 1)) * SB + (row & (SB - 1)), fill)
        key, low, w_sorted = lax.sort((key, low, jnp.pad(w, fill)), num_keys=1, is_stable=False)
        key_rows = key.reshape(-1, LANES)
        end = jnp.full((8,), none, jnp.int32)
        k_first = jnp.concatenate([jnp.min(key_rows, axis=1), end])
        k_last = jnp.concatenate([jnp.max(key_rows, axis=1), end])
        rows_of = lambda a: a.reshape(-1, 1, LANES)
        edges = (k_first, k_last, rows_of(key), rows_of(low), rows_of(w_sorted))

        owner = over(hub_ids, verts)
        ids = jnp.arange(hubs)
        earlier = (owner[None, :] == owner[:, None]) & (ids[None, :] < ids[:, None])
        place = owner * own_hubs + jnp.sum(earlier.astype(jnp.int32), axis=1)
        place_half = lax.dynamic_slice_in_dim(place, col * k_half, k_half)
        slot_ids = me * own_hubs + jnp.arange(own_hubs)
        my_rows = jnp.sum(jnp.where(place[None, :] == slot_ids[:, None], hub_ids[None, :], 0), axis=1) - me * verts
        my_line = jnp.pad(my_rows, (0, LANES - own_hubs), constant_values=-1)[None, :]
        wanted = jnp.where(send_valid > 0, send_idx, -1)
        wanted = lax.dynamic_slice_in_dim(wanted, col * s_half, s_half, 1).reshape(-1)
        across = lambda a: jnp.broadcast_to(a[:, None], (a.shape[0], LANES))
        lists = (across(wanted), across(my_rows))

        z = jnp.dot(x_loc, w1[0], preferred_element_type=F32)
        z = (z + jnp.dot(lax.ppermute(x_loc, "feat", swap), w1[1], preferred_element_type=F32)).astype(BF)
        table = first_table(n_graph, z, *lists, across(place_half), depth)
        adjacency, mine, other = build_and_multiply(edges, table, hub_blocks + local_blocks)
        weights = jnp.concatenate(w2, axis=0)
        return rest(
            n_graph, mine, other, adjacency, weights, b_first[None, :], b_second[None, :],
            *lists, my_line, across(place_half), place[None, :],
        )

    edge = P(rows_axes)
    send = P(rows_axes, None)
    in_specs = (P(rows_axes, "feat"), edge, edge, edge, edge, send, send, P("data"), P("feat", None), P("feat", None), P("feat"), P("feat"))
    return jax.shard_map(device_program, mesh=mesh, in_specs=in_specs, out_specs=P(rows_axes, "feat"), check_vma=False)
```
